256 devices in a mesh: dp: 4 (over x), seq: 64 (over y, z, core).
Axes of the slice: x: 4, y: 4, z: 8, core: 2. Of those that a mesh axis runs over, the one named last changes fastest.
Arguments:
- tiles: bfloat16 [4, 65536, 768], P('dp', 'seq'), may hold values from -48 to 48
- tile_count: int32 [4], P('dp'), may hold values from 32769 to 65536
- offsets: int32 [16], replicated, may hold values from 0 to 15
- w_query: bfloat16 [768, 768], replicated, may hold values from -0.375 to 0.375
- w_key: bfloat16 [768, 768], replicated, may hold values from -0.375 to 0.375
- w_value: bfloat16 [768, 768], replicated, may hold values from -0.21875 to 0.21875
- w_out: bfloat16 [768, 768], replicated, may hold values from -0.21875 to 0.21875
- cotangent: bfloat16 [4, 65536, 768], P('dp', 'seq'), may hold values from -0.03125 to 0.03125
Outputs:
- branch: bfloat16 [4, 65536, 768], P('dp', 'seq')
- grad_out: float32 [768, 768], P(None, 'seq')
The draws below stay inside these ranges and needn't reach their ends.
All inputs are finite; a program needn't handle non-finite values.
Results may differ from the reference program's by a relative error of at most 0.0095.
The reference program's roundings to bfloat16 on the way count: a program that leaves them out, or rounds other values in their place, can miss the bound.
Values may be sent and summed in bfloat16 or wider, within the bound.
No kernel may reach another device: no remote copies, remote signals or barrier semaphores. Data moves between devices by JAX's collectives and lax.ppermute only.
A program may use at most 128 MiB of HBM per device.

```python
import jax
import jax.numpy as jnp
from jax import lax

D = 768
ATTENTION_HEADS = 16
HEAD_SIZE = 48
SEG = 1024
RATE = 16
SLIDES = 4
TOKENS = 65536


def draw_tiles(key, part):
    extent = (SLIDES, TOKENS, D)
    normal_key = jax.random.fold_in(key, 0)
    values = jax.random.truncated_normal(normal_key, -6.0, 6.0, extent, jnp.float32)
    return values.astype(jnp.bfloat16)


def plant(entries, key, least, high):
    longest = entries.shape.index(max(entries.shape))
    spots = []
    for shift in (0, 1):
        where = [jax.random.randint(jax.random.fold_in(key, axis), (), 0, length) for axis, length in enumerate(entries.shape)]
        where[longest] = (where[longest] + shift) % entries.shape[longest]
        spots.append(tuple(where))
    return entries.at[spots[0]].set(least).at[spots[1]].set(high)


def raised(drawn, key, source, target, parts, factor):
    def block_of(dim):
        return (jnp.arange(drawn.shape[dim]) // (drawn.shape[dim] // parts)).reshape((-1,) + (1,) * (drawn.ndim - 1 - dim))

    first = jax.random.permutation(key, parts)[block_of(target)]
    other_side = (block_of(target) + parts // 2) % parts
    return jnp.where((block_of(source) == first) | (block_of(source) == other_side), factor * drawn, drawn)


def block_scale(key, shape, shards, low, top_value):
    def one(dim, parts):
        draws = jax.random.uniform(jax.random.fold_in(jax.random.fold_in(key, 6), dim), (parts,), jnp.float32, low / len(shards), top_value / len(shards))
        return jnp.repeat(jnp.exp(draws), shape[dim] // parts).reshape((-1,) + (1,) * (len(shape) - dim - 1))

    factor_of = one(*shards[0])
    for cut in shards[1:]:
        factor_of = factor_of * one(*cut)
    return factor_of


def bell_draw(own_key, dims, scale, limit, pieces=(), held_as=jnp.bfloat16):
    array = jax.random.normal(own_key, dims, jnp.float32) * scale
    if len(pieces) > 0:
        array = block_scale(own_key, dims, pieces, -0.22, 0.18) * array
    return jnp.clip(array, min=-limit, max=limit).astype(held_as)


def gaussian_with(key, shape, scale, bound, pieces, heavy, kind=jnp.bfloat16):
    array = scale * jax.random.normal(key, shape, jnp.float32)
    if pieces:
        array = array * block_scale(key, shape, pieces, -0.22, 0.18)
    return jnp.clip(raised(array, jax.random.fold_in(key, 3), *heavy), -bound, bound).astype(kind)


def setup_inputs(seed: int = 0) -> dict:
    arg_keys = jax.random.split(jax.random.key(seed), 9)
    return {
        "tiles": draw_tiles(jax.random.fold_in(arg_keys[8], 71), 0),
        "tile_count": plant(jax.random.randint(arg_keys[1], (SLIDES,), TOKENS // 2 + 1, TOKENS + 1), jax.random.fold_in(arg_keys[1], 1), TOKENS // 2 + 1, TOKENS).astype(jnp.int32),
        "offsets": plant(jax.random.randint(arg_keys[2], (ATTENTION_HEADS,), 0, RATE), jax.random.fold_in(arg_keys[2], 1), 0, RATE - 1).astype(jnp.int32),
        "w_query": bell_draw(arg_keys[3], (D, D), (D // 3) ** -0.5, 0.375),
        "w_key": bell_draw(arg_keys[4], (D, D), (D // 3) ** -0.5, 0.375),
        "w_value": bell_draw(arg_keys[5], (D, D), D ** -0.5, 0.21875),
        "w_out": bell_draw(arg_keys[6], (D, D), D ** -0.5, 0.21875),
        "cotangent": gaussian_with(arg_keys[7], (SLIDES, TOKENS, D), (TOKENS * SLIDES) ** -0.5, 0.03125, ((0, 4), (1, 64)), (1, 2, 64, 4.0)),
    }


NEGATIVE_FLOOR = -1e30


def project(inputs, weight):
    return jnp.dot(inputs, weight, preferred_element_type=jnp.float32).astype(jnp.bfloat16)


def select_rows(tensor, offsets):
    segment_height = tensor.shape[0]
    grouped = tensor.reshape(segment_height // RATE, RATE, ATTENTION_HEADS, HEAD_SIZE).astype(jnp.float32)
    onehot = (jnp.arange(RATE, dtype=jnp.int32)[:, None] == offsets[None, :]).astype(jnp.float32)
    return jnp.einsum('arhd,rh->ahd', grouped, onehot).astype(jnp.bfloat16)


def segment_attention(blocks):
    query_seg, key_seg, value_seg, alive_seg = blocks
    scores = jnp.einsum('qhd,khd->hqk', query_seg.astype(jnp.float32), key_seg.astype(jnp.float32)) * (HEAD_SIZE ** -0.5)
    scores = jnp.where(alive_seg[None, None, :], scores, NEGATIVE_FLOOR)
    maxima = jnp.max(scores, axis=-1)
    weights = jnp.exp(scores - maxima[..., None])
    totals = jnp.sum(weights, axis=-1)
    rounded = lax.optimization_barrier(weights.astype(jnp.bfloat16))
    weighted = jnp.einsum('hqk,khd->qhd', rounded.astype(jnp.float32), value_seg.astype(jnp.float32))
    return maxima.T, totals.T, weighted


def combine(local, dilated_branch, offsets, is_live):
    local_max, local_total, local_sum = local
    dilated_row_max, dilated_value_total, dilated_row_sum = dilated_branch
    segment_height = local_max.shape[0]
    dilation_match = jnp.arange(RATE, dtype=jnp.int32)[:, None] == offsets[None, :]
    dense_row_max = jnp.where(dilation_match[None], dilated_row_max[:, None, :], NEGATIVE_FLOOR).reshape(segment_height, ATTENTION_HEADS)
    dense_value_total = jnp.where(dilation_match[None], dilated_value_total[:, None, :], 0.0).reshape(segment_height, ATTENTION_HEADS)
    dense_row_sum = jnp.where(dilation_match[None, :, :, None], dilated_row_sum[:, None], 0.0).reshape(segment_height, ATTENTION_HEADS, HEAD_SIZE)
    top = jnp.maximum(local_max, dense_row_max)
    near = jnp.exp(local_max - top)
    far = jnp.exp(dense_row_max - top)
    attn = (near[..., None] * local_sum + far[..., None] * dense_row_sum) / (near * local_total + far * dense_value_total)[..., None]
    attn = jnp.where(is_live[:, None, None], attn, 0.0)
    return attn.reshape(segment_height, D).astype(jnp.bfloat16)


def reference(tiles, tile_count, offsets, w_query, w_key, w_value, w_out, cotangent):
    outputs = []
    gradient = jnp.zeros((D, D), jnp.float32)
    segments = TOKENS // SEG
    picked = TOKENS // RATE
    for slide in range(SLIDES):
        inputs = tiles[slide]
        live_count = tile_count[slide]
        query_proj = project(inputs, w_query).reshape(TOKENS, ATTENTION_HEADS, HEAD_SIZE)
        key_proj = project(inputs, w_key).reshape(TOKENS, ATTENTION_HEADS, HEAD_SIZE)
        value_proj = project(inputs, w_value).reshape(TOKENS, ATTENTION_HEADS, HEAD_SIZE)
        is_live = jnp.arange(TOKENS, dtype=jnp.int32) < live_count
        local = lax.map(segment_attention, (query_proj.reshape(segments, SEG, ATTENTION_HEADS, HEAD_SIZE), key_proj.reshape(segments, SEG, ATTENTION_HEADS, HEAD_SIZE), value_proj.reshape(segments, SEG, ATTENTION_HEADS, HEAD_SIZE), is_live.reshape(segments, SEG)))
        local = (local[0].reshape(TOKENS, ATTENTION_HEADS), local[1].reshape(TOKENS, ATTENTION_HEADS), local[2].reshape(TOKENS, ATTENTION_HEADS, HEAD_SIZE))
        query_sel = select_rows(query_proj, offsets).transpose(1, 0, 2)
        key_sel = select_rows(key_proj, offsets).transpose(1, 0, 2)
        value_sel = select_rows(value_proj, offsets).transpose(1, 0, 2)

        def head_attention(blocks):
            query_head, key_head, value_head, offset = blocks
            key_live = jnp.arange(picked, dtype=jnp.int32) * RATE + offset < live_count
            scores = jnp.dot(query_head, key_head.T, preferred_element_type=jnp.float32) * (HEAD_SIZE ** -0.5)
            scores = jnp.where(key_live[None, :], scores, NEGATIVE_FLOOR)
            maxima = jnp.max(scores, axis=-1)
            weights = jnp.exp(scores - maxima[:, None])
            totals = jnp.sum(weights, axis=-1)
            weighted = jnp.dot(weights.astype(jnp.bfloat16), value_head, preferred_element_type=jnp.float32)
            return maxima, totals, weighted

        dilated_branch = lax.map(head_attention, (query_sel, key_sel, value_sel, offsets))
        dilated_branch = (dilated_branch[0].T, dilated_branch[1].T, dilated_branch[2].transpose(1, 0, 2))
        attn = combine(local, dilated_branch, offsets, is_live)
        outputs.append(jnp.dot(attn, w_out, preferred_element_type=jnp.float32).astype(jnp.bfloat16))
        gradient = gradient + jnp.dot(attn.T, cotangent[slide], preferred_element_type=jnp.float32)
    return jnp.stack(outputs), gradient
```

```python
import jax
import jax.numpy as jnp
from jax import lax
from jax.experimental import pallas as pl
from jax.experimental.pallas import tpu as pltpu
from jax.sharding import PartitionSpec as P

D = 768
HEADS = 16
HEAD = 48
SEG = 1024
RATE = 16
PICKED = SEG // RATE
PAIRS = HEADS // 2
SHARDS = 64
QUARTER = PICKED // 4
FLOOR = -1e30
LOG2E = 1.4426950408889634
SCALE2 = HEAD ** (-0.5) * LOG2E

f32 = jnp.float32
bf16 = jnp.bfloat16


def lanes(shape):
    return lax.broadcasted_iota(jnp.int32, shape, len(shape) - 1)


def rows(shape):
    return lax.broadcasted_iota(jnp.int32, shape, len(shape) - 2)


def nt(a, b):
    return lax.dot_general(a, b, (((1,), (1,)), ((), ())), preferred_element_type=f32)


def nn(a, b):
    return jnp.dot(a, b, preferred_element_type=f32)


def pick_kernel(x_ref, wq_ref, wk_ref, wv_ref, off_ref, send_ref, x2_ref):
    i = rows((256, 256))
    c = lanes((256, 256))
    onehot = ((i % 16 == c // 16) & (c % 16 == off_ref[...])).astype(bf16)
    for b in range(4):
        y = nn(onehot, x_ref[b * 256 : (b + 1) * 256, :]).astype(bf16)
        for h in range(HEADS):
            x2_ref[h * 64 + b * 16 : h * 64 + b * 16 + 16, :] = y[h * 16 : (h + 1) * 16, :]
    sel = []
    col = lanes((64, 256))
    for w_ref in (wq_ref, wk_ref, wv_ref):
        parts = []
        for t in range(3):
            y = nn(x2_ref[320 * t : 320 * t + 384, :], w_ref[:, 256 * t : 256 * t + 256])
            out = y[0:64]
            for k in range(1, 6):
                start = (5 * t + k) * HEAD - 256 * t
                out = jnp.where(col >= start, y[64 * k : 64 * k + 64], out)
            parts.append(out)
        sel.append(jnp.concatenate(parts, axis=1))
    q, k, v = sel
    lane = lanes((64, 128))
    for h in range(HEADS):
        t = min(48 * h // 128, 4)
        o = 48 * h - 128 * t

        def moved(a, to):
            return pltpu.roll(a[:, 128 * t : 128 * t + 256], (to - o) % 256, 1)[:, :128]

        kv = jnp.where(lane < 48, moved(k, 0), moved(v, 48))
        q_low = moved(q, 96)
        q_high = moved(q, 64)
        for j in range(4):
            s = slice(16 * j, 16 * j + 16)
            mine = jnp.concatenate([q_low[s], q_high[s], q_low[0:32]], axis=0)
            send_ref[4 * h + j] = jnp.where(lane < 96, kv, mine).astype(bf16)


def pick(x, wq, wk, wv, off256):
    return pl.pallas_call(
        pick_kernel,
        out_shape=jax.ShapeDtypeStruct((SHARDS, PICKED, 128), bf16),
        scratch_shapes=[pltpu.VMEM((1024, D), bf16)],
        compiler_params=pltpu.CompilerParams(vmem_limit_bytes=40 << 20),
        name="pick",
    )(x, wq, wk, wv, off256)


def local_kernel(scal_ref, off_ref, x_ref, wq_ref, wk_ref, wv_ref, attn_ref, so_ref, sl_ref, o_s, l_s):
    p = pl.program_id(0)
    t = jnp.minimum((3 * p) // 4, 4)
    shift = 96 * p - 128 * t
    wl = lanes((D, 128))

    def weight(ref):
        w = ref[:, pl.ds(pl.multiple_of(128 * t, 128), 256)].astype(f32)
        w = pltpu.roll(w, 256 - shift, 1)[:, :128]
        return jnp.where(wl < 96, w, 0.0).astype(bf16)

    w = jnp.concatenate([weight(wq_ref), weight(wk_ref), weight(wv_ref)], axis=1)
    qkv = nn(x_ref[...], w)
    lane = lanes((SEG, 128))
    live = rows((SEG, 128)) + scal_ref[1] < scal_ref[0]
    q = jnp.where(lane == 96, 1.0, qkv[:, 0:128]).astype(bf16)
    bias = jnp.where(live, 0.0, FLOOR)
    kf = jnp.where(lane == 96, bias, qkv[:, 128:256])
    v = jnp.concatenate([qkv[:, 256:384], jnp.ones((SEG, 128), f32)], axis=1).astype(bf16)
    bl = lanes((256, 128))
    for b in range(4):
        r = slice(256 * b, 256 * b + 256)
        both = []
        for a in range(2):
            inside = (lane < 48) if a == 0 else ((lane >= 48) & (lane < 96))
            kh = jnp.where(inside | (lane == 96), kf, 0.0).astype(bf16)
            s = nt(q[r], kh)
            m = jnp.max(s, axis=1, keepdims=True)
            e = jnp.exp2((s - m) * SCALE2).astype(bf16)
            o = nn(e, v)
            total = o[:, 128:256]
            both.append((o[:, 0:128] / total, m * SCALE2 + jnp.log2(total)))
        out = jnp.where(bl < 48, both[0][0], both[1][0])
        attn_ref[0, r, :] = out.astype(bf16)
        o_s[r, :] = out
        l_s[r, :] = jnp.where(bl < 48, both[0][1], both[1][1])
    sel = lanes((PICKED, 128)) < 48
    first = pl.ds(off_ref[2 * p], PICKED, stride=RATE)
    second = pl.ds(off_ref[2 * p + 1], PICKED, stride=RATE)
    so_ref[0] = jnp.where(sel, o_s[first, :], o_s[second, :])
    sl_ref[0] = jnp.where(sel, l_s[first, :], l_s[second, :])


def local(scal, offsets, x, wq, wk, wv):
    whole = lambda shape: pl.BlockSpec(shape, lambda p, *_: (0,) * len(shape), pipeline_mode=pl.Buffered(1))
    return pl.pallas_call(
        local_kernel,
        grid_spec=pltpu.PrefetchScalarGridSpec(
            num_scalar_prefetch=2,
            grid=(PAIRS,),
            in_specs=[whole((SEG, D)), whole((D, D)), whole((D, D)), whole((D, D))],
            out_specs=[
                pl.BlockSpec((1, SEG, 128), lambda p, *_: (p, 0, 0)),
                pl.BlockSpec((1, PICKED, 128), lambda p, *_: (p, 0, 0)),
                pl.BlockSpec((1, PICKED, 128), lambda p, *_: (p, 0, 0)),
            ],
            scratch_shapes=[pltpu.VMEM((SEG, 128), f32), pltpu.VMEM((SEG, 128), f32)],
        ),
        out_shape=[
            jax.ShapeDtypeStruct((PAIRS, SEG, 128), bf16),
            jax.ShapeDtypeStruct((PAIRS, PICKED, 128), f32),
            jax.ShapeDtypeStruct((PAIRS, PICKED, 128), f32),
        ],
        compiler_params=pltpu.CompilerParams(
            dimension_semantics=("arbitrary",), vmem_limit_bytes=48 << 20
        ),
        cost_estimate=pl.CostEstimate(flops=24_000_000_000, transcendentals=16 << 20, bytes_accessed=8 << 20),
        name="local",
    )(scal, offsets, x, wq, wk, wv)


def cot_kernel(perm_ref, cot_ref, out_ref):
    onehot = (lanes((D, D)) == perm_ref[...]).astype(bf16)
    out_ref[...] = nt(onehot, cot_ref[...]).astype(bf16)


def cot_prep(perm, cot):
    return pl.pallas_call(
        cot_kernel,
        out_shape=jax.ShapeDtypeStruct((D, SEG), bf16),
        compiler_params=pltpu.CompilerParams(vmem_limit_bytes=40 << 20),
        cost_estimate=pl.CostEstimate(flops=1_500_000_000, transcendentals=0, bytes_accessed=4 << 20),
        name="cotangent",
    )(perm, cot)


def far_kernel(scal_ref, recv_ref, ret_ref, kb_s, v_s, q_s):
    kv = recv_ref[...].reshape(SHARDS * PICKED, 128).astype(f32)
    lane = lanes(kv.shape)
    live = rows(kv.shape) * RATE + scal_ref[2] < scal_ref[0]
    kb_s[...] = jnp.where(lane == 112, jnp.where(live, 0.0, FLOOR), kv).astype(bf16)
    v_s[:, 0:128] = kv.astype(bf16)
    v_s[:, 128:256] = jnp.ones(kv.shape, bf16)
    low = recv_ref[:, 0:16, :].reshape(SEG, 128).astype(f32)
    high = recv_ref[:, 16:32, :].reshape(SEG, 128).astype(f32)
    ql = lanes((SEG, 128))
    q = jnp.where(ql < 32, pltpu.roll(low, 32, 1), pltpu.roll(high, 64, 1))
    q_s[...] = jnp.where(ql < 48, q, jnp.where(ql == 112, 1.0, 0.0)).astype(bf16)
    bl = lanes((256, 128))
    hl = lanes((16, 8, 128))
    for b in range(4):
        s = nt(q_s[256 * b : 256 * b + 256, :], kb_s[...])
        m = jnp.max(s, axis=1, keepdims=True)
        e = jnp.exp2((s - m) * SCALE2).astype(bf16)
        o = nn(e, v_s[...])
        total = o[:, 128:256]
        out = pltpu.roll(o[:, 0:128] / total, 80, 1)
        level = m * SCALE2 + jnp.log2(total)
        part0 = level.astype(bf16).astype(f32)
        part1 = (level - part0).astype(bf16).astype(f32)
        part2 = level - part0 - part1
        out = jnp.where(bl < 48, out, jnp.where(bl == 48, part0, jnp.where(bl == 49, part1, part2)))
        out = out.reshape(16, 16, 128)
        second = pltpu.roll(out[:, 8:16, :], 64, 2)
        ret_ref[16 * b : 16 * b + 16] = jnp.where(hl < 64, out[:, 0:8, :], second).astype(bf16)


def far(scal, recv):
    return pl.pallas_call(
        far_kernel,
        in_specs=[pl.BlockSpec(memory_space=pltpu.SMEM), pl.BlockSpec(memory_space=pltpu.VMEM)],
        out_shape=jax.ShapeDtypeStruct((SHARDS, 8, 128), bf16),
        scratch_shapes=[
            pltpu.VMEM((SHARDS * PICKED, 128), bf16),
            pltpu.VMEM((SHARDS * PICKED, 256), bf16),
            pltpu.VMEM((SEG, 128), bf16),
        ],
        compiler_params=pltpu.CompilerParams(vmem_limit_bytes=56 << 20),
        cost_estimate=pl.CostEstimate(flops=6_000_000_000, transcendentals=4 << 20, bytes_accessed=2 << 20),
        name="far",
    )(scal, recv)


def natural(pair, n):
    lane = lanes((n, 128))
    out = []
    for t in range(6):
        p = 128 * t // 96
        o = 128 * t - 96 * p
        n0 = 96 - o
        a = pair(p)
        a = pltpu.roll(a, 128 - o, 1) if o else a
        out.append(jnp.where(lane < n0, a, pltpu.roll(pair(p + 1), n0, 1)))
    return jnp.concatenate(out, axis=1)


def merge_kernel(scal_ref, offcol_ref, attn_ref, so_ref, sl_ref, ret_ref, wout_ref, cot_ref, branch_ref, grad_ref, attn_s):
    lane = lanes((PICKED, 128))
    merged = []
    for p in range(PAIRS):
        tiles, levels = [], []
        for h in (2 * p, 2 * p + 1):
            pieces = []
            for j in range(4):
                block = ret_ref[4 * h + j].astype(f32)
                pieces += [block, pltpu.roll(block, 64, 1)]
            tile = jnp.concatenate(pieces, axis=0)
            tiles.append(tile)
            levels.append(tile[:, 48:49] + tile[:, 49:50] + tile[:, 50:51])
        value = jnp.where(lane < 48, tiles[0], pltpu.roll(tiles[1], 48, 1))
        gap = jnp.where(lane < 48, levels[0], levels[1]) - sl_ref[p]
        near = 1.0 / (1.0 + jnp.exp2(gap))
        distant = 1.0 / (1.0 + jnp.exp2(-gap))
        merged.append(near * so_ref[p] + distant * value)
    sel = natural(lambda p: merged[p], PICKED).astype(bf16)
    wout = wout_ref[...]
    for b in range(4):
        r = slice(256 * b, 256 * b + 256)
        spread = (rows((256, PICKED)) // RATE + 16 * b == lanes((256, PICKED))).astype(bf16)
        far_rows = nn(spread, sel)
        near_rows = natural(lambda p: attn_ref[p, r, :].astype(f32), 256)
        row = rows((256, D))
        attn = jnp.where(row % RATE == offcol_ref[...], far_rows, near_rows)
        attn = jnp.where(row + (scal_ref[1] + 256 * b) < scal_ref[0], attn, 0.0).astype(bf16)
        attn_s[r, :] = attn
        branch_ref[r, :] = nn(attn, wout).astype(bf16)
    grad_ref[...] = nn(cot_ref[...], attn_s[...]).astype(bf16)


def merge(scal, offcol, attn, so, sl, ret, wout, cot):
    v = pl.BlockSpec(memory_space=pltpu.VMEM)
    return pl.pallas_call(
        merge_kernel,
        in_specs=[pl.BlockSpec(memory_space=pltpu.SMEM)] + [v] * 7,
        out_shape=[jax.ShapeDtypeStruct((SEG, D), bf16), jax.ShapeDtypeStruct((D, D), bf16)],
        scratch_shapes=[pltpu.VMEM((SEG, D), bf16)],
        compiler_params=pltpu.CompilerParams(vmem_limit_bytes=40 << 20),
        cost_estimate=pl.CostEstimate(flops=4_000_000_000, transcendentals=0, bytes_accessed=8 << 20),
        name="merge",
    )(scal, offcol, attn, so, sl, ret, wout, cot)


def place(y, z, c):
    return (y * 8 + z) * 2 + c


EVERY = [(y, z, c) for y in range(4) for z in range(8) for c in range(2)]
Z_GROUPS = [[place(y, z, c) for z in range(8)] for y in range(4) for c in range(2)]


def to_partner(a):
    return lax.ppermute(a, "seq", [(place(y, z, c), place(y, z, 1 - c)) for y, z, c in EVERY])


def along_y(a, k):
    return lax.ppermute(a, "seq", [(place(y, z, c), place((y + k) % 4, z, c)) for y, z, c in EVERY])


def across_slides(a, k):
    return lax.ppermute(a, "dp", [(x, x ^ k) for x in range(4)])


def reduce_gradient(grad):
    got = to_partner(grad[D // 2 :])
    half = (grad[: D // 2].astype(f32) + got.astype(f32)).astype(bf16)
    got = [along_y(half[96 * k : 96 * k + 96], k) for k in (1, 2, 3)]
    part = half[:96].astype(f32) + got[0].astype(f32) + (got[1].astype(f32) + got[2].astype(f32))
    blocks = part.astype(bf16).reshape(8, 12, D)
    blocks = lax.all_to_all(blocks, "seq", 0, 0, tiled=True, axis_index_groups=Z_GROUPS)
    mine = blocks.astype(f32).sum(axis=0)
    got = [across_slides(mine, k) for k in (1, 2, 3)]
    return ((mine + got[0]) + (got[1] + got[2])).T


def body(tiles, tile_count, offsets, w_query, w_key, w_value, w_out, cotangent):
    x = tiles[0]
    rank = lax.axis_index("seq")
    y, z, c = rank // 16, (rank // 2) % 8, rank % 2
    offset = lax.dynamic_index_in_dim(offsets, rank // 4, 0, keepdims=False)
    scal = jnp.stack([tile_count[0], rank * SEG, offset])
    off256 = jnp.repeat(offsets, 16)[:, None]
    offcol = jnp.repeat(offsets, HEAD)[None, :]
    n = jnp.arange(D, dtype=jnp.int32)
    to_c = c ^ (n // 384)
    to_y = (y + (n // 96) % 4) % 4
    to_z = (n // 12) % 8
    perm = ((to_y * 8 + to_z) * 2 + to_c) * 12 + n % 12

    send = pick(x, w_query, w_key, w_value, off256)
    recv = lax.all_to_all(send, "seq", 0, 0, tiled=True)
    attn, so, sl = local(scal, offsets, x, w_query, w_key, w_value)
    cot = cot_prep(perm[:, None], cotangent[0])
    ret = far(scal, recv)
    back = lax.all_to_all(ret, "seq", 0, 0, tiled=True)
    branch, grad = merge(scal, offcol, attn, so, sl, back, w_out, cot)
    return branch[None], reduce_gradient(grad)


def solution(mesh):
    in_specs = (P("dp", "seq", None), P("dp"), P(), P(), P(), P(), P(), P("dp", "seq", None))
    out_specs = (P("dp", "seq", None), P(None, "seq"))
    return jax.shard_map(body, mesh=mesh, in_specs=in_specs, out_specs=out_specs, check_vma=False)
```

```python
import functools

import jax
import jax.numpy as jnp
from jax import lax
from jax.experimental import pallas as pl
from jax.experimental.pallas import tpu as pltpu
from jax.sharding import PartitionSpec as P

D = 768
HEADS = 16
HEAD = 48
SEG = 1024
RATE = 16
PICKED = SEG // RATE
PAIRS = HEADS // 2
SHARDS = 64
EARLY = 3
FLOOR = -1e30
LOCAL_VMEM = 28 << 20
LOG2E = 1.4426950408889634
SCALE2 = HEAD ** (-0.5) * LOG2E

f32 = jnp.float32
bf16 = jnp.bfloat16


def lanes(shape):
    return lax.broadcasted_iota(jnp.int32, shape, len(shape) - 1)


def rows(shape):
    return lax.broadcasted_iota(jnp.int32, shape, len(shape) - 2)


def hbm(a):
    return pltpu.with_memory_space_constraint(a, pltpu.HBM)


def vmem(a):
    return pltpu.with_memory_space_constraint(a, pltpu.VMEM)


def nt(a, b):
    return lax.dot_general(a, b, (((1,), (1,)), ((), ())), preferred_element_type=f32)


def nn(a, b):
    return jnp.dot(a, b, preferred_element_type=f32)


HBM = pl.BlockSpec(memory_space=pltpu.HBM)
SMEM = pl.BlockSpec(memory_space=pltpu.SMEM)
VMEM = pl.BlockSpec(memory_space=pltpu.VMEM)


def pick_kernel(off_ref, x_hbm, wq_hbm, wk_hbm, wv_hbm, send_ref, x_ref, w_ref, x2_ref, sems):
    copies = []
    for b in range(4):
        r = pl.ds(256 * b, 256)
        copies.append(pltpu.make_async_copy(x_hbm.at[r], x_ref.at[r], sems.at[b]))
    for n, hbm in enumerate((wq_hbm, wk_hbm, wv_hbm)):
        for t in range(3):
            r = pl.ds(256 * t, 256)
            copies.append(pltpu.make_async_copy(hbm.at[:, r], w_ref.at[n, :, r], sems.at[4 + 3 * n + t]))
    for copy in copies:
        copy.start()
    c = lanes((16, 256))
    same = c // 16 == rows((16, 256))
    onehot = jnp.concatenate([(same & (c % 16 == off_ref[h])).astype(f32) for h in range(HEADS)], axis=0).astype(bf16)
    for b in range(4):
        copies[b].wait()
        y = nn(onehot, x_ref[b * 256 : (b + 1) * 256, :]).astype(bf16)
        for h in range(HEADS):
            x2_ref[h * 64 + b * 16 : h * 64 + b * 16 + 16, :] = y[h * 16 : (h + 1) * 16, :]
    sel = []
    col = lanes((64, 256))
    for n in range(3):
        parts = []
        for t in range(3):
            copies[4 + 3 * n + t].wait()
            y = nn(x2_ref[320 * t : 320 * t + 384, :], w_ref[n, :, 256 * t : 256 * t + 256])
            out = y[0:64]
            for k in range(1, 6):
                start = (5 * t + k) * HEAD - 256 * t
                out = jnp.where(col >= start, y[64 * k : 64 * k + 64], out)
            parts.append(out)
        sel.append(jnp.concatenate(parts, axis=1))
    q, k, v = sel
    lane = lanes((64, 128))
    for h in range(HEADS):
        t = min(48 * h // 128, 4)
        o = 48 * h - 128 * t

        def moved(a, to):
            return pltpu.roll(a[:, 128 * t : 128 * t + 256], (to - o) % 256, 1)[:, :128]

        kv = jnp.where(lane < 48, moved(k, 0), moved(v, 48))
        q_low = moved(q, 96)
        q_high = moved(q, 64)
        for j in range(4):
            s = slice(16 * j, 16 * j + 16)
            mine = jnp.concatenate([q_low[s], q_high[s], q_low[0:32]], axis=0)
            send_ref[4 * h + j] = jnp.where(lane < 96, kv, mine).astype(bf16)


def pick(offsets, x, wq, wk, wv):
    return pl.pallas_call(
        pick_kernel,
        in_specs=[SMEM, HBM, HBM, HBM, HBM],
        out_shape=[
            jax.ShapeDtypeStruct((SHARDS, PICKED, 128), bf16),
            pltpu.VMEM((SEG, D), bf16),
        ],
        out_specs=[VMEM, VMEM],
        scratch_shapes=[
            pltpu.VMEM((3, D, D), bf16),
            pltpu.VMEM((SEG, D), bf16),
            pltpu.SemaphoreType.DMA((13,)),
        ],
        compiler_params=pltpu.CompilerParams(vmem_limit_bytes=24 << 20),
        name="pick",
    )(offsets, hbm(x), hbm(wq), hbm(wk), hbm(wv))


def local_kernel(first, groups, rank_ref, count_ref, off_ref, x_ref, wq_hbm, wk_hbm, wv_hbm, *refs):
    step = pl.program_id(0)
    if first == 0:
        cot_hbm, attn_ref, so_ref, sl_ref, out_hbm, w_ref, o_s, l_s, cot_s, out_s, sems = refs
        load = pltpu.make_async_copy(cot_hbm, cot_s, sems.at[18])
        store = pltpu.make_async_copy(out_s, out_hbm, sems.at[19])
    else:
        attn_ref, so_ref, sl_ref, w_ref, o_s, l_s, sems = refs
    tiles = {g: [3 * g // 2, 3 * g // 2 + 1] for g in range(first, first + groups)}
    windows = {}
    for g, new in tiles.items():
        for u in new:
            if u not in windows:
                r = pl.ds(128 * u, 128)
                windows[u] = (g - first, [
                    pltpu.make_async_copy(hbm.at[:, r], w_ref.at[n, :, r], sems.at[3 * u + n])
                    for n, hbm in enumerate((wq_hbm, wk_hbm, wv_hbm))
                ])

    @pl.when(step == 0)
    def _():
        for _, copies in windows.values():
            for copy in copies:
                copy.start()
        if first == 0:
            load.start()

    for at, copies in windows.values():

        @pl.when(step == at)
        def _(copies=copies):
            for copy in copies:
                copy.wait()

    here = 2 * step
    g = step + first
    t = (3 * g) // 2
    shift = 192 * g - 128 * t
    wl = lanes((D, 128))
    weights = []
    for part in range(2):
        for n in range(3):
            w = w_ref[n, :, pl.ds(pl.multiple_of(128 * t, 128), 256)].astype(f32)
            w = pltpu.roll(w, 256 - 96 * part - shift, 1)[:, :128]
            weights.append(jnp.where(wl < 96, w, 0.0).astype(bf16))
    qkv = nn(x_ref[...], jnp.concatenate(weights, axis=1))
    lane = lanes((SEG, 128))
    live = rows((SEG, 128)) + rank_ref[0] * SEG < count_ref[0]
    bias = jnp.where(live, 0.0, FLOOR)
    ones = jnp.ones((SEG, 128), f32)
    bl = lanes((256, 128))
    sel = lanes((PICKED, 128)) < 48
    for part in range(2):
        qf, kf, vf = (qkv[:, 384 * part + 128 * n : 384 * part + 128 * n + 128] for n in range(3))
        q = jnp.where(lane == 96, 1.0, qf).astype(bf16)
        kf = jnp.where(lane == 96, bias, kf)
        v = jnp.concatenate([vf, ones], axis=1).astype(bf16)
        inside = (lane < 48, (lane >= 48) & (lane < 96))
        kh = [jnp.where(i | (lane == 96), kf, 0.0).astype(bf16) for i in inside]
        for b in range(4):
            r = slice(256 * b, 256 * b + 256)
            both = []
            for a in range(2):
                s = nt(q[r], kh[a])
                m = jnp.max(s, axis=1, keepdims=True)
                e = jnp.exp2((s - m) * SCALE2).astype(bf16)
                o = nn(e, v)
                total = o[:, 128:256]
                both.append((o[:, 0:128] / total, m * SCALE2 + jnp.log2(total)))
            out = jnp.where(bl < 48, both[0][0], both[1][0])
            attn_ref[part, r, :] = out.astype(bf16)
            o_s[part, r, :] = out
            l_s[part, r, :] = jnp.where(bl < 48, both[0][1], both[1][1])
        even = pl.ds(off_ref[4 * g + 2 * part], PICKED, stride=RATE)
        odd = pl.ds(off_ref[4 * g + 2 * part + 1], PICKED, stride=RATE)
        so_ref[here + part] = jnp.where(sel, o_s[part, even, :], o_s[part, odd, :])
        sl_ref[here + part] = jnp.where(sel, l_s[part, even, :], l_s[part, odd, :])


    if first == 0:

        @pl.when(step == 1)
        def _():
            load.wait()
            reorder_cotangent(rank_ref[0], cot_s, out_s)
            store.start()

        @pl.when(step == groups - 1)
        def _():
            store.wait()


def reorder_cotangent(rank, cot_ref, out_ref):
    y, c = rank // 16, rank % 2
    n = rows((96, D))
    offset = lanes((96, D)) - n - 12 * ((n * 171) // 2048)

    def half(i, carry):
        blocks = []
        for k in range(4):
            owner = ((y + k) % 4) * 16 + (c + i) % 2
            blocks.append((offset == 12 * owner).astype(f32))
        onehot = jnp.concatenate(blocks, axis=0).astype(bf16)
        out_ref[pl.ds(pl.multiple_of(384 * i, 384), 384), :] = nt(onehot, cot_ref[...]).astype(bf16)
        return carry

    lax.fori_loop(0, 2, half, 0)


def local(first, groups, rank, count, offsets, x, weights, cot=None):
    out_specs = [pl.BlockSpec((2, SEG, 128), lambda p: (p, 0, 0)), VMEM, VMEM]
    out_shape = [
        pltpu.HBM((2 * groups, SEG, 128), bf16),
        pltpu.VMEM((2 * groups, PICKED, 128), f32),
        pltpu.VMEM((2 * groups, PICKED, 128), f32),
    ]
    scratch = [pltpu.VMEM((3, D, D), bf16), pltpu.VMEM((2, SEG, 128), f32), pltpu.VMEM((2, SEG, 128), f32)]
    operands = (rank, count, offsets, vmem(x), *(hbm(w) for w in weights))
    in_specs = [SMEM, SMEM, SMEM, VMEM, HBM, HBM, HBM]
    if first == 0:
        out_specs.append(HBM)
        out_shape.append(pltpu.HBM((D, SEG), bf16))
        scratch += [pltpu.VMEM((SEG, D), bf16), pltpu.VMEM((D, SEG), bf16)]
        operands += (hbm(cot),)
        in_specs.append(HBM)
    scratch.append(pltpu.SemaphoreType.DMA((20,)))
    return pl.pallas_call(
        functools.partial(local_kernel, first, groups),
        grid=(groups,),
        in_specs=in_specs,
        out_specs=out_specs,
        out_shape=out_shape,
        scratch_shapes=scratch,
        compiler_params=pltpu.CompilerParams(
            dimension_semantics=("arbitrary",), vmem_limit_bytes=LOCAL_VMEM
        ),
        cost_estimate=pl.CostEstimate(flops=6_000_000_000 * groups, transcendentals=groups << 22, bytes_accessed=8 << 20),
        name="local",
    )(*operands)


def far_kernel(rank_ref, count_ref, off_ref, recv_ref, ret_ref, after_ref, kb_s, v_s, q_s):
    after_ref[0] = count_ref[0]
    kv = recv_ref[...].reshape(SHARDS * PICKED, 128).astype(f32)
    lane = lanes(kv.shape)
    live = rows(kv.shape) * RATE + off_ref[rank_ref[0] // 4] < count_ref[0]
    kb_s[...] = jnp.where(lane == 112, jnp.where(live, 0.0, FLOOR), kv).astype(bf16)
    v_s[:, 0:128] = kv.astype(bf16)
    v_s[:, 128:256] = jnp.ones(kv.shape, bf16)
    low = recv_ref[:, 0:16, :].reshape(SEG, 128).astype(f32)
    high = recv_ref[:, 16:32, :].reshape(SEG, 128).astype(f32)
    ql = lanes((SEG, 128))
    q = jnp.where(ql < 32, pltpu.roll(low, 32, 1), pltpu.roll(high, 64, 1))
    q_s[...] = jnp.where(ql < 48, q, jnp.where(ql == 112, 1.0, 0.0)).astype(bf16)
    bl = lanes((256, 128))
    hl = lanes((16, 8, 128))
    for b in range(4):
        s = nt(q_s[256 * b : 256 * b + 256, :], kb_s[...])
        m = jnp.max(s, axis=1, keepdims=True)
        e = jnp.exp2((s - m) * SCALE2).astype(bf16)
        o = nn(e, v_s[...])
        total = o[:, 128:256]
        out = pltpu.roll(o[:, 0:128] / total, 80, 1)
        level = m * SCALE2 + jnp.log2(total)
        part0 = level.astype(bf16).astype(f32)
        part1 = (level - part0).astype(bf16).astype(f32)
        part2 = level - part0 - part1
        out = jnp.where(bl < 48, out, jnp.where(bl == 48, part0, jnp.where(bl == 49, part1, part2)))
        out = out.reshape(16, 16, 128)
        second = pltpu.roll(out[:, 8:16, :], 64, 2)
        ret_ref[16 * b : 16 * b + 16] = jnp.where(hl < 64, out[:, 0:8, :], second).astype(bf16)


def far(rank, count, offsets, recv):
    return pl.pallas_call(
        far_kernel,
        in_specs=[SMEM, SMEM, SMEM, VMEM],
        out_specs=[VMEM, SMEM],
        out_shape=[jax.ShapeDtypeStruct((SHARDS, 8, 128), bf16), jax.ShapeDtypeStruct((1,), jnp.int32)],
        scratch_shapes=[
            pltpu.VMEM((SHARDS * PICKED, 128), bf16),
            pltpu.VMEM((SHARDS * PICKED, 256), bf16),
            pltpu.VMEM((SEG, 128), bf16),
        ],
        compiler_params=pltpu.CompilerParams(vmem_limit_bytes=32 << 20),
        cost_estimate=pl.CostEstimate(flops=6_000_000_000, transcendentals=4 << 20, bytes_accessed=2 << 20),
        name="far",
    )(rank, count, offsets, recv)


def natural(pair, n):
    lane = lanes((n, 128))
    out = []
    for t in range(6):
        p = 128 * t // 96
        o = 128 * t - 96 * p
        n0 = 96 - o
        a = pair(p)
        a = pltpu.roll(a, 128 - o, 1) if o else a
        out.append(jnp.where(lane < n0, a, pltpu.roll(pair(p + 1), n0, 1)))
    return jnp.concatenate(out, axis=1)


def merge_kernel(split, rank_ref, count_ref, off_ref, attn0_hbm, attn1_hbm, so0_ref, so1_ref, sl0_ref, sl1_ref, ret_ref, wout_hbm, cot_hbm, branch_hbm, grad_ref, near_s, cot_s, attn_s, wout_s, branch_s, sems):
    loads = []
    for b in range(4):
        part = pl.ds(256 * b, 256)
        loads.append([
            pltpu.make_async_copy(attn0_hbm.at[:, part], near_s.at[0:split, part], sems.at[6 + 2 * b]),
            pltpu.make_async_copy(attn1_hbm.at[:, part], near_s.at[split:PAIRS, part], sems.at[7 + 2 * b]),
        ])
    load = pltpu.make_async_copy(wout_hbm, wout_s, sems.at[4])
    last_load = pltpu.make_async_copy(cot_hbm, cot_s, sems.at[5])
    for copy in (*loads[0], load, *loads[1], *loads[2], *loads[3], last_load):
        copy.start()
    either = lambda early, late, p: early.at[p] if p < split else late.at[p - split]
    lane = lanes((PICKED, 128))
    merged = []
    for p in range(PAIRS):
        tiles, levels = [], []
        for h in (2 * p, 2 * p + 1):
            pieces = []
            for j in range(4):
                block = ret_ref[4 * h + j].astype(f32)
                pieces += [block, pltpu.roll(block, 64, 1)]
            tile = jnp.concatenate(pieces, axis=0)
            tiles.append(tile)
            levels.append(tile[:, 48:49] + tile[:, 49:50] + tile[:, 50:51])
        value = jnp.where(lane < 48, tiles[0], pltpu.roll(tiles[1], 48, 1))
        gap = jnp.where(lane < 48, levels[0], levels[1]) - either(sl0_ref, sl1_ref, p)[...]
        near = 1.0 / (1.0 + jnp.exp2(gap))
        distant = 1.0 / (1.0 + jnp.exp2(-gap))
        merged.append(near * either(so0_ref, so1_ref, p)[...] + distant * value)
    sel = natural(lambda p: merged[p], PICKED).astype(bf16)
    col = lanes((8, D))
    offcol = jnp.zeros((8, D), jnp.int32)
    for h in range(HEADS):
        offcol = jnp.where(col >= HEAD * h, off_ref[h], offcol)
    offcol = offcol[0:1]
    stores = []
    for b in range(4):
        r = slice(256 * b, 256 * b + 256)
        spread = (rows((256, PICKED)) // RATE + 16 * b == lanes((256, PICKED))).astype(bf16)
        far_rows = nn(spread, sel)
        for copy in loads[b]:
            copy.wait()
        near_rows = natural(lambda p: near_s[p, r, :].astype(f32), 256)
        row = rows((256, D))
        attn = jnp.where(row % RATE == offcol, far_rows, near_rows)
        attn = jnp.where(row + (rank_ref[0] * SEG + 256 * b) < count_ref[0], attn, 0.0).astype(bf16)
        attn_s[r, :] = attn
        if b == 0:
            load.wait()
        branch_s[r, :] = nn(attn, wout_s[...]).astype(bf16)
        part = pl.ds(256 * b, 256)
        stores.append(pltpu.make_async_copy(branch_s.at[part], branch_hbm.at[part], sems.at[b]))
        stores[b].start()
    last_load.wait()

    def half(i, carry):
        part = pl.ds(pl.multiple_of(384 * i, 384), 384)
        grad_ref[part, :] = nn(cot_s[part, :], attn_s[...]).astype(bf16)
        return carry

    lax.fori_loop(0, 2, half, 0)
    for store in stores:
        store.wait()


def merge(rank, count, offsets, near0, near1, ret, wout, cot):
    split = near0[0].shape[0]
    return pl.pallas_call(
        functools.partial(merge_kernel, split),
        in_specs=[SMEM] * 3 + [HBM] * 2 + [VMEM] * 5 + [HBM] * 2,
        out_specs=[HBM, VMEM],
        out_shape=[jax.ShapeDtypeStruct((SEG, D), bf16), jax.ShapeDtypeStruct((D, D), bf16)],
        scratch_shapes=[
            pltpu.VMEM((PAIRS, SEG, 128), bf16),
            pltpu.VMEM((D, SEG), bf16),
            pltpu.VMEM((SEG, D), bf16),
            pltpu.VMEM((D, D), bf16),
            pltpu.VMEM((SEG, D), bf16),
            pltpu.SemaphoreType.DMA((14,)),
        ],
        compiler_params=pltpu.CompilerParams(vmem_limit_bytes=20 << 20),
        cost_estimate=pl.CostEstimate(flops=4_000_000_000, transcendentals=0, bytes_accessed=8 << 20),
        name="merge",
    )(rank, count, offsets, hbm(near0[0]), hbm(near1[0]), *(vmem(a) for n in (1, 2) for a in (near0[n], near1[n])), vmem(ret), hbm(wout), hbm(cot))


def place(y, z, c):
    return (y * 8 + z) * 2 + c


EVERY = [(y, z, c) for y in range(4) for z in range(8) for c in range(2)]
Z_GROUPS = [[place(y, z, c) for z in range(8)] for y in range(4) for c in range(2)]


def to_partner(a):
    return lax.ppermute(a, "seq", [(place(y, z, c), place(y, z, 1 - c)) for y, z, c in EVERY])


def along_y(a, k):
    return lax.ppermute(a, "seq", [(place(y, z, c), place((y + k) % 4, z, c)) for y, z, c in EVERY])


def across_slides(a, k):
    return lax.ppermute(a, "dp", [(x, x ^ k) for x in range(4)])


def reduce_gradient(grad):
    got = to_partner(grad[D // 2 :])
    half = (grad[: D // 2].astype(f32) + got.astype(f32)).astype(bf16)
    got = [along_y(half[96 * k : 96 * k + 96], k) for k in (1, 2, 3)]
    part = half[:96].astype(f32) + got[0].astype(f32) + (got[1].astype(f32) + got[2].astype(f32))
    blocks = part.astype(bf16).reshape(8, 12, D)
    blocks = lax.all_to_all(blocks, "seq", 0, 0, tiled=True, axis_index_groups=Z_GROUPS)
    mine = blocks.astype(f32).sum(axis=0)
    got = [across_slides(mine, k) for k in (1, 2, 3)]
    return ((mine + got[0]) + (got[1] + got[2])).T


def body(tiles, tile_count, offsets, w_query, w_key, w_value, w_out, cotangent):
    x = tiles[0]
    rank = lax.axis_index("seq")
    rank = rank.astype(jnp.int32)[None]
    weights = (w_query, w_key, w_value)
    send, x = pick(offsets, x, *weights)
    recv = lax.all_to_all(send, "seq", 0, 0, tiled=True)
    *near0, cot = local(0, EARLY, rank, tile_count, offsets, x, weights, cotangent[0])
    ret, after = far(rank, tile_count, offsets, recv)
    back = lax.all_to_all(ret, "seq", 0, 0, tiled=True)
    near1 = local(EARLY, 4 - EARLY, rank, after, offsets, x, weights)
    branch, grad = merge(rank, tile_count, offsets, near0, near1, back, w_out, cot)
    return branch[None], reduce_gradient(grad)


def solution(mesh):
    in_specs = (P("dp", "seq", None), P("dp"), P(), P(), P(), P(), P(), P("dp", "seq", None))
    out_specs = (P("dp", "seq", None), P(None, "seq"))
    return jax.shard_map(body, mesh=mesh, in_specs=in_specs, out_specs=out_specs, check_vma=False)
```

```python
import functools

import jax
import jax.numpy as jnp
from jax import lax
from jax.experimental import pallas as pl
from jax.experimental.pallas import tpu as pltpu
from jax.sharding import PartitionSpec as P


D = 768
HEADS = 16
HEAD = 48
SEG = 1024
RATE = 16
PICKED = SEG // RATE
PAIRS = HEADS // 2
SHARDS = 64
EARLY = 3
FLOOR = -1e30
LOCAL_VMEM = 28 << 20
BRANCH_VMEM = 16 << 20
LOG2E = 1.4426950408889634
SCALE2 = HEAD ** (-0.5) * LOG2E

f32 = jnp.float32
bf16 = jnp.bfloat16


def lanes(shape):
    return lax.broadcasted_iota(jnp.int32, shape, len(shape) - 1)


def rows(shape):
    return lax.broadcasted_iota(jnp.int32, shape, len(shape) - 2)


def hbm(a):
    return pltpu.with_memory_space_constraint(a, pltpu.HBM)


def vmem(a):
    return pltpu.with_memory_space_constraint(a, pltpu.VMEM)


def nt(a, b):
    return lax.dot_general(a, b, (((1,), (1,)), ((), ())), preferred_element_type=f32)


def nn(a, b):
    return jnp.dot(a, b, preferred_element_type=f32)


HBM = pl.BlockSpec(memory_space=pltpu.HBM)
SMEM = pl.BlockSpec(memory_space=pltpu.SMEM)
VMEM = pl.BlockSpec(memory_space=pltpu.VMEM)


def pick_kernel(off_ref, x_hbm, wq_hbm, wk_hbm, wv_hbm, send_ref, x_ref, w_ref, x2_ref, sems):
    copies = []
    for b in range(4):
        r = pl.ds(256 * b, 256)
        copies.append(pltpu.make_async_copy(x_hbm.at[r], x_ref.at[r], sems.at[b]))
    for n, hbm in enumerate((wq_hbm, wk_hbm, wv_hbm)):
        for t in range(3):
            r = pl.ds(256 * t, 256)
            copies.append(pltpu.make_async_copy(hbm.at[:, r], w_ref.at[n, :, r], sems.at[4 + 3 * n + t]))
    for copy in copies:
        copy.start()
    c = lanes((16, 256))
    same = c // 16 == rows((16, 256))
    onehot = jnp.concatenate([(same & (c % 16 == off_ref[h])).astype(f32) for h in range(HEADS)], axis=0).astype(bf16)
    for b in range(4):
        copies[b].wait()
        y = nn(onehot, x_ref[b * 256 : (b + 1) * 256, :]).astype(bf16)
        for h in range(HEADS):
            x2_ref[h * 64 + b * 16 : h * 64 + b * 16 + 16, :] = y[h * 16 : (h + 1) * 16, :]
    sel = []
    col = lanes((64, 256))
    for n in range(3):
        parts = []
        for t in range(3):
            copies[4 + 3 * n + t].wait()
            y = nn(x2_ref[320 * t : 320 * t + 384, :], w_ref[n, :, 256 * t : 256 * t + 256])
            out = y[0:64]
            for k in range(1, 6):
                start = (5 * t + k) * HEAD - 256 * t
                out = jnp.where(col >= start, y[64 * k : 64 * k + 64], out)
            parts.append(out)
        sel.append(jnp.concatenate(parts, axis=1))
    q, k, v = sel
    lane = lanes((64, 128))
    for h in range(HEADS):
        t = min(48 * h // 128, 4)
        o = 48 * h - 128 * t

        def moved(a, to):
            return pltpu.roll(a[:, 128 * t : 128 * t + 256], (to - o) % 256, 1)[:, :128]

        kv = jnp.where(lane < 48, moved(k, 0), moved(v, 48))
        q_low = moved(q, 96)
        q_high = moved(q, 64)
        for j in range(4):
            s = slice(16 * j, 16 * j + 16)
            mine = jnp.concatenate([q_low[s], q_high[s], q_low[0:32]], axis=0)
            send_ref[4 * h + j] = jnp.where(lane < 96, kv, mine).astype(bf16)


def pick(offsets, x, wq, wk, wv):
    return pl.pallas_call(
        pick_kernel,
        in_specs=[SMEM, HBM, HBM, HBM, HBM],
        out_shape=[
            jax.ShapeDtypeStruct((SHARDS, PICKED, 128), bf16),
            pltpu.VMEM((SEG, D), bf16),
        ],
        out_specs=[VMEM, VMEM],
        scratch_shapes=[
            pltpu.VMEM((3, D, D), bf16),
            pltpu.VMEM((SEG, D), bf16),
            pltpu.SemaphoreType.DMA((13,)),
        ],
        compiler_params=pltpu.CompilerParams(vmem_limit_bytes=24 << 20),
        name="pick",
    )(hbm(offsets), hbm(x), hbm(wq), hbm(wk), hbm(wv))


def local_kernel(first, groups, rank_ref, count_ref, off_ref, x_ref, wq_hbm, wk_hbm, wv_hbm, *refs):
    step = pl.program_id(0)
    if first == 0:
        cot_hbm, attn_ref, so_ref, sl_ref, out_hbm, w_ref, o_s, l_s, cot_s, out_s, sems = refs
        load = pltpu.make_async_copy(cot_hbm, cot_s, sems.at[18])
        store = pltpu.make_async_copy(out_s, out_hbm, sems.at[19])
    else:
        attn_ref, so_ref, sl_ref, w_ref, o_s, l_s, sems = refs
    tiles = {g: [3 * g // 2, 3 * g // 2 + 1] for g in range(first, first + groups)}
    windows = {}
    for g, new in tiles.items():
        for u in new:
            if u not in windows:
                r = pl.ds(128 * u, 128)
                windows[u] = (g - first, [
                    pltpu.make_async_copy(hbm.at[:, r], w_ref.at[n, :, r], sems.at[3 * u + n])
                    for n, hbm in enumerate((wq_hbm, wk_hbm, wv_hbm))
                ])

    @pl.when(step == 0)
    def _():
        for _, copies in windows.values():
            for copy in copies:
                copy.start()
        if first == 0:
            load.start()

    for at, copies in windows.values():

        @pl.when(step == at)
        def _(copies=copies):
            for copy in copies:
                copy.wait()

    here = 2 * step
    g = step + first
    t = (3 * g) // 2
    shift = 192 * g - 128 * t
    wl = lanes((D, 128))
    weights = []
    for part in range(2):
        for n in range(3):
            w = w_ref[n, :, pl.ds(pl.multiple_of(128 * t, 128), 256)].astype(f32)
            w = pltpu.roll(w, 256 - 96 * part - shift, 1)[:, :128]
            weights.append(jnp.where(wl < 96, w, 0.0).astype(bf16))
    qkv = nn(x_ref[...], jnp.concatenate(weights, axis=1))
    lane = lanes((SEG, 128))
    live = rows((SEG, 128)) + rank_ref[0] * SEG < count_ref[0]
    bias = jnp.where(live, 0.0, FLOOR)
    ones = jnp.ones((SEG, 128), f32)
    bl = lanes((256, 128))
    sel = lanes((PICKED, 128)) < 48
    for part in range(2):
        qf, kf, vf = (qkv[:, 384 * part + 128 * n : 384 * part + 128 * n + 128] for n in range(3))
        q = jnp.where(lane == 96, 1.0, qf).astype(bf16)
        kf = jnp.where(lane == 96, bias, kf)
        v = jnp.concatenate([vf, ones], axis=1).astype(bf16)
        inside = (lane < 48, (lane >= 48) & (lane < 96))
        kh = [jnp.where(i | (lane == 96), kf, 0.0).astype(bf16) for i in inside]
        for b in range(4):
            r = slice(256 * b, 256 * b + 256)
            both = []
            for a in range(2):
                s = nt(q[r], kh[a])
                m = jnp.max(s, axis=1, keepdims=True)
                e = jnp.exp2((s - m) * SCALE2).astype(bf16)
                o = nn(e, v)
                total = o[:, 128:256]
                both.append((o[:, 0:128] / total, m * SCALE2 + jnp.log2(total)))
            out = jnp.where(bl < 48, both[0][0], both[1][0])
            attn_ref[part, r, :] = out.astype(bf16)
            o_s[part, r, :] = out
            l_s[part, r, :] = jnp.where(bl < 48, both[0][1], both[1][1])
        even = pl.ds(off_ref[4 * g + 2 * part], PICKED, stride=RATE)
        odd = pl.ds(off_ref[4 * g + 2 * part + 1], PICKED, stride=RATE)
        so_ref[here + part] = jnp.where(sel, o_s[part, even, :], o_s[part, odd, :])
        sl_ref[here + part] = jnp.where(sel, l_s[part, even, :], l_s[part, odd, :])


    if first == 0:

        @pl.when(step == 1)
        def _():
            load.wait()
            reorder_cotangent(rank_ref[0], cot_s, out_s)
            store.start()

        @pl.when(step == groups - 1)
        def _():
            store.wait()


def reorder_cotangent(rank, cot_ref, out_ref):
    y, c = rank // 16, rank % 2
    n = rows((96, D))
    offset = lanes((96, D)) - n - 12 * ((n * 171) // 2048)

    def half(i, carry):
        blocks = []
        for k in range(4):
            owner = ((y + k) % 4) * 16 + (c + i) % 2
            blocks.append((offset == 12 * owner).astype(f32))
        onehot = jnp.concatenate(blocks, axis=0).astype(bf16)
        out_ref[pl.ds(pl.multiple_of(384 * i, 384), 384), :] = nt(onehot, cot_ref[...]).astype(bf16)
        return carry

    lax.fori_loop(0, 2, half, 0)


def local(first, groups, rank, count, offsets, x, weights, cot=None):
    out_specs = [pl.BlockSpec((2, SEG, 128), lambda p: (p, 0, 0)), VMEM, VMEM]
    out_shape = [
        pltpu.HBM((2 * groups, SEG, 128), bf16),
        pltpu.VMEM((2 * groups, PICKED, 128), f32),
        pltpu.VMEM((2 * groups, PICKED, 128), f32),
    ]
    scratch = [pltpu.VMEM((3, D, D), bf16), pltpu.VMEM((2, SEG, 128), f32), pltpu.VMEM((2, SEG, 128), f32)]
    operands = (rank, count, offsets, vmem(x), *(hbm(w) for w in weights))
    in_specs = [SMEM, SMEM, SMEM, VMEM, HBM, HBM, HBM]
    if first == 0:
        out_specs.append(HBM)
        out_shape.append(pltpu.HBM((D, SEG), bf16))
        scratch += [pltpu.VMEM((SEG, D), bf16), pltpu.VMEM((D, SEG), bf16)]
        operands += (hbm(cot),)
        in_specs.append(HBM)
    scratch.append(pltpu.SemaphoreType.DMA((20,)))
    return pl.pallas_call(
        functools.partial(local_kernel, first, groups),
        grid=(groups,),
        in_specs=in_specs,
        out_specs=out_specs,
        out_shape=out_shape,
        scratch_shapes=scratch,
        compiler_params=pltpu.CompilerParams(
            dimension_semantics=("arbitrary",), vmem_limit_bytes=LOCAL_VMEM
        ),
        cost_estimate=pl.CostEstimate(flops=6_000_000_000 * groups, transcendentals=groups << 22, bytes_accessed=8 << 20),
        name="local",
    )(*operands)


def far_kernel(rank_ref, count_ref, off_ref, recv_ref, ret_ref, after_ref, kb_s, v_s, q_s):
    after_ref[0] = count_ref[0]
    kv = recv_ref[...].reshape(SHARDS * PICKED, 128).astype(f32)
    lane = lanes(kv.shape)
    live = rows(kv.shape) * RATE + off_ref[rank_ref[0] // 4] < count_ref[0]
    kb_s[...] = jnp.where(lane == 112, jnp.where(live, 0.0, FLOOR), kv).astype(bf16)
    v_s[:, 0:128] = kv.astype(bf16)
    v_s[:, 128:256] = jnp.ones(kv.shape, bf16)
    low = recv_ref[:, 0:16, :].reshape(SEG, 128).astype(f32)
    high = recv_ref[:, 16:32, :].reshape(SEG, 128).astype(f32)
    ql = lanes((SEG, 128))
    q = jnp.where(ql < 32, pltpu.roll(low, 32, 1), pltpu.roll(high, 64, 1))
    q_s[...] = jnp.where(ql < 48, q, jnp.where(ql == 112, 1.0, 0.0)).astype(bf16)
    bl = lanes((256, 128))
    hl = lanes((16, 8, 128))
    for b in range(4):
        s = nt(q_s[256 * b : 256 * b + 256, :], kb_s[...])
        m = jnp.max(s, axis=1, keepdims=True)
        e = jnp.exp2((s - m) * SCALE2).astype(bf16)
        o = nn(e, v_s[...])
        total = o[:, 128:256]
        out = pltpu.roll(o[:, 0:128] / total, 80, 1)
        level = m * SCALE2 + jnp.log2(total)
        part0 = level.astype(bf16).astype(f32)
        part1 = (level - part0).astype(bf16).astype(f32)
        part2 = level - part0 - part1
        out = jnp.where(bl < 48, out, jnp.where(bl == 48, part0, jnp.where(bl == 49, part1, part2)))
        out = out.reshape(16, 16, 128)
        second = pltpu.roll(out[:, 8:16, :], 64, 2)
        ret_ref[16 * b : 16 * b + 16] = jnp.where(hl < 64, out[:, 0:8, :], second).astype(bf16)


def far(rank, count, offsets, recv):
    return pl.pallas_call(
        far_kernel,
        in_specs=[SMEM, SMEM, SMEM, VMEM],
        out_specs=[VMEM, SMEM],
        out_shape=[jax.ShapeDtypeStruct((SHARDS, 8, 128), bf16), jax.ShapeDtypeStruct((1,), jnp.int32)],
        scratch_shapes=[
            pltpu.VMEM((SHARDS * PICKED, 128), bf16),
            pltpu.VMEM((SHARDS * PICKED, 256), bf16),
            pltpu.VMEM((SEG, 128), bf16),
        ],
        compiler_params=pltpu.CompilerParams(vmem_limit_bytes=32 << 20),
        cost_estimate=pl.CostEstimate(flops=6_000_000_000, transcendentals=4 << 20, bytes_accessed=2 << 20),
        name="far",
    )(rank, count, offsets, recv)


def natural(pair, n):
    lane = lanes((n, 128))
    out = []
    for t in range(6):
        p = 128 * t // 96
        o = 128 * t - 96 * p
        n0 = 96 - o
        a = pair(p)
        a = pltpu.roll(a, 128 - o, 1) if o else a
        out.append(jnp.where(lane < n0, a, pltpu.roll(pair(p + 1), n0, 1)))
    return jnp.concatenate(out, axis=1)


def merge_kernel(split, rank_ref, count_ref, off_ref, attn0_hbm, attn1_hbm, so0_ref, so1_ref, sl0_ref, sl1_ref, ret_ref, cot_hbm, attn_hbm, grad_ref, near_s, cot_s, attn_s, sems):
    loads = []
    for b in range(4):
        part = pl.ds(256 * b, 256)
        loads.append([
            pltpu.make_async_copy(attn0_hbm.at[:, part], near_s.at[0:split, part], sems.at[6 + 2 * b]),
            pltpu.make_async_copy(attn1_hbm.at[:, part], near_s.at[split:PAIRS, part], sems.at[7 + 2 * b]),
        ])
    last_load = pltpu.make_async_copy(cot_hbm, cot_s, sems.at[5])
    for copy in (*loads[0], *loads[1], *loads[2], *loads[3], last_load):
        copy.start()
    either = lambda early, late, p: early.at[p] if p < split else late.at[p - split]
    lane = lanes((PICKED, 128))
    merged = []
    for p in range(PAIRS):
        tiles, levels = [], []
        for h in (2 * p, 2 * p + 1):
            pieces = []
            for j in range(4):
                block = ret_ref[4 * h + j].astype(f32)
                pieces += [block, pltpu.roll(block, 64, 1)]
            tile = jnp.concatenate(pieces, axis=0)
            tiles.append(tile)
            levels.append(tile[:, 48:49] + tile[:, 49:50] + tile[:, 50:51])
        value = jnp.where(lane < 48, tiles[0], pltpu.roll(tiles[1], 48, 1))
        gap = jnp.where(lane < 48, levels[0], levels[1]) - either(sl0_ref, sl1_ref, p)[...]
        near = 1.0 / (1.0 + jnp.exp2(gap))
        distant = 1.0 / (1.0 + jnp.exp2(-gap))
        merged.append(near * either(so0_ref, so1_ref, p)[...] + distant * value)
    sel = natural(lambda p: merged[p], PICKED).astype(bf16)
    col = lanes((8, D))
    offcol = jnp.zeros((8, D), jnp.int32)
    for h in range(HEADS):
        offcol = jnp.where(col >= HEAD * h, off_ref[h], offcol)
    offcol = offcol[0:1]
    stores = []
    for b in range(4):
        r = slice(256 * b, 256 * b + 256)
        spread = (rows((256, PICKED)) // RATE + 16 * b == lanes((256, PICKED))).astype(bf16)
        far_rows = nn(spread, sel)
        for copy in loads[b]:
            copy.wait()
        near_rows = natural(lambda p: near_s[p, r, :].astype(f32), 256)
        row = rows((256, D))
        attn = jnp.where(row % RATE == offcol, far_rows, near_rows)
        attn = jnp.where(row + (rank_ref[0] * SEG + 256 * b) < count_ref[0], attn, 0.0).astype(bf16)
        attn_s[r, :] = attn
        part = pl.ds(256 * b, 256)
        stores.append(pltpu.make_async_copy(attn_s.at[part], attn_hbm.at[part], sems.at[b]))
        stores[b].start()
    last_load.wait()

    def half(i, carry):
        part = pl.ds(pl.multiple_of(384 * i, 384), 384)
        grad_ref[part, :] = nn(cot_s[part, :], attn_s[...]).astype(bf16)
        return carry

    lax.fori_loop(0, 2, half, 0)
    for store in stores:
        store.wait()


def merge(rank, count, offsets, near0, near1, ret, cot):
    split = near0[0].shape[0]
    return pl.pallas_call(
        functools.partial(merge_kernel, split),
        in_specs=[SMEM] * 3 + [HBM] * 2 + [VMEM] * 5 + [HBM],
        out_specs=[HBM, VMEM],
        out_shape=[pltpu.HBM((SEG, D), bf16), jax.ShapeDtypeStruct((D, D), bf16)],
        scratch_shapes=[
            pltpu.VMEM((PAIRS, SEG, 128), bf16),
            pltpu.VMEM((D, SEG), bf16),
            pltpu.VMEM((SEG, D), bf16),
            pltpu.SemaphoreType.DMA((14,)),
        ],
        compiler_params=pltpu.CompilerParams(vmem_limit_bytes=20 << 20),
        cost_estimate=pl.CostEstimate(flops=4_000_000_000, transcendentals=0, bytes_accessed=8 << 20),
        name="merge",
    )(rank, count, offsets, hbm(near0[0]), hbm(near1[0]), *(vmem(a) for n in (1, 2) for a in (near0[n], near1[n])), vmem(ret), hbm(cot))


def branch_kernel(attn_ref, wout_ref, branch_ref):
    branch_ref[...] = nn(attn_ref[...], wout_ref[...]).astype(bf16)


def project_out(attn, wout):
    rows_of = pl.BlockSpec((256, D), lambda b: (b, 0))
    return pl.pallas_call(
        branch_kernel,
        grid=(4,),
        in_specs=[rows_of, pl.BlockSpec((D, D), lambda b: (0, 0))],
        out_specs=rows_of,
        out_shape=jax.ShapeDtypeStruct((SEG, D), bf16),
        compiler_params=pltpu.CompilerParams(dimension_semantics=("arbitrary",), vmem_limit_bytes=BRANCH_VMEM),
        cost_estimate=pl.CostEstimate(flops=1_300_000_000, transcendentals=0, bytes_accessed=5 << 20),
        name="branch",
    )(hbm(attn), hbm(wout))


def place(y, z, c):
    return (y * 8 + z) * 2 + c


EVERY = [(y, z, c) for y in range(4) for z in range(8) for c in range(2)]
Z_GROUPS = [[place(y, z, c) for z in range(8)] for y in range(4) for c in range(2)]


def to_partner(a):
    return lax.ppermute(a, "seq", [(place(y, z, c), place(y, z, 1 - c)) for y, z, c in EVERY])


def along_y(a, k):
    return lax.ppermute(a, "seq", [(place(y, z, c), place((y + k) % 4, z, c)) for y, z, c in EVERY])


def across_slides(a, k):
    return lax.ppermute(a, "dp", [(x, x ^ k) for x in range(4)])


def reduce_gradient(grad):
    got = to_partner(grad[D // 2 :])
    half = (grad[: D // 2].astype(f32) + got.astype(f32)).astype(bf16)
    blocks = [half[96 * k : 96 * k + 96] for k in (1, 2, 3)]
    got = [along_y(blocks[k - 1], k) for k in (1, 2, 3)]
    part = half[:96].astype(f32) + got[0].astype(f32) + (got[1].astype(f32) + got[2].astype(f32))
    blocks = part.astype(bf16).reshape(8, 12, D)
    blocks = lax.all_to_all(blocks, "seq", 0, 0, tiled=True, axis_index_groups=Z_GROUPS)
    mine = blocks.astype(f32).sum(axis=0)
    got = [across_slides(mine, k) for k in (1, 2, 3)]
    return ((mine + got[0]) + (got[1] + got[2])).T


def body(tiles, tile_count, offsets, w_query, w_key, w_value, w_out, cotangent):
    x = tiles[0]
    rank = lax.axis_index("seq")
    rank = rank.astype(jnp.int32)[None]
    weights = (w_query, w_key, w_value)
    send, x = pick(offsets, x, *weights)
    recv = lax.all_to_all(send, "seq", 0, 0, tiled=True)
    *near0, cot = local(0, EARLY, rank, tile_count, offsets, x, weights, cotangent[0])
    ret, after = far(rank, tile_count, offsets, recv)
    back = lax.all_to_all(ret, "seq", 0, 0, tiled=True)
    near1 = local(EARLY, 4 - EARLY, rank, after, offsets, x, weights)
    attn, grad = merge(rank, tile_count, offsets, near0, near1, back, cot)
    branch = project_out(attn, w_out)
    return branch[None], reduce_gradient(grad)


def solution(mesh):
    in_specs = (P("dp", "seq", None), P("dp"), P(), P(), P(), P(), P(), P("dp", "seq", None))
    out_specs = (P("dp", "seq", None), P(None, "seq"))
    return jax.shard_map(body, mesh=mesh, in_specs=in_specs, out_specs=out_specs, check_vma=False)
```

```python
import functools

import jax
import jax.numpy as jnp
from jax import lax
from jax.experimental import pallas as pl
from jax.experimental.pallas import tpu as pltpu
from jax.sharding import PartitionSpec as P


D = 768
HEADS = 16
HEAD = 48
SEG = 1024
RATE = 16
PICKED = SEG // RATE
PAIRS = HEADS // 2
SHARDS = 64
EARLY = 3
FLOOR = -1e30
LOCAL_VMEM = 28 << 20
BRANCH_VMEM = 16 << 20
LOG2E = 1.4426950408889634
SCALE2 = HEAD ** (-0.5) * LOG2E

f32 = jnp.float32
bf16 = jnp.bfloat16


def lanes(shape):
    return lax.broadcasted_iota(jnp.int32, shape, len(shape) - 1)


def rows(shape):
    return lax.broadcasted_iota(jnp.int32, shape, len(shape) - 2)


def hbm(a):
    return pltpu.with_memory_space_constraint(a, pltpu.HBM)


def vmem(a):
    return pltpu.with_memory_space_constraint(a, pltpu.VMEM)


def nt(a, b):
    return lax.dot_general(a, b, (((1,), (1,)), ((), ())), preferred_element_type=f32)


def nn(a, b):
    return jnp.dot(a, b, preferred_element_type=f32)


HBM = pl.BlockSpec(memory_space=pltpu.HBM)
SMEM = pl.BlockSpec(memory_space=pltpu.SMEM)
VMEM = pl.BlockSpec(memory_space=pltpu.VMEM)


def pick_kernel(off_ref, x_hbm, wq_hbm, wk_hbm, wv_hbm, send_hbm, x_ref, w_ref, x2_ref, send_ref, sems):
    copies = []
    for b in range(4):
        r = pl.ds(256 * b, 256)
        copies.append(pltpu.make_async_copy(x_hbm.at[r], x_ref.at[r], sems.at[b]))
    for n, hbm in enumerate((wq_hbm, wk_hbm, wv_hbm)):
        for t in range(3):
            r = pl.ds(256 * t, 256)
            copies.append(pltpu.make_async_copy(hbm.at[:, r], w_ref.at[n, :, r], sems.at[4 + 3 * n + t]))
    for copy in copies:
        copy.start()
    c = lanes((16, 256))
    same = c // 16 == rows((16, 256))
    onehot = jnp.concatenate([(same & (c % 16 == off_ref[h])).astype(f32) for h in range(HEADS)], axis=0).astype(bf16)
    for b in range(4):
        copies[b].wait()
        y = nn(onehot, x_ref[b * 256 : (b + 1) * 256, :]).astype(bf16)
        for h in range(HEADS):
            x2_ref[h * 64 + b * 16 : h * 64 + b * 16 + 16, :] = y[h * 16 : (h + 1) * 16, :]
    sel = []
    col = lanes((64, 256))
    for n in range(3):
        parts = []
        for t in range(3):
            copies[4 + 3 * n + t].wait()
            y = nn(x2_ref[320 * t : 320 * t + 384, :], w_ref[n, :, 256 * t : 256 * t + 256])
            out = y[0:64]
            for k in range(1, 6):
                start = (5 * t + k) * HEAD - 256 * t
                out = jnp.where(col >= start, y[64 * k : 64 * k + 64], out)
            parts.append(out)
        sel.append(jnp.concatenate(parts, axis=1))
    q, k, v = sel
    lane = lanes((64, 128))
    stores = []
    for h in range(HEADS):
        t = min(48 * h // 128, 4)
        o = 48 * h - 128 * t

        def moved(a, to):
            return pltpu.roll(a[:, 128 * t : 128 * t + 256], (to - o) % 256, 1)[:, :128]

        kv = jnp.where(lane < 48, moved(k, 0), moved(v, 48))
        q_low = moved(q, 96)
        q_high = moved(q, 64)
        for j in range(4):
            s = slice(16 * j, 16 * j + 16)
            mine = jnp.concatenate([q_low[s], q_high[s], q_low[0:32]], axis=0)
            send_ref[4 * h + j] = jnp.where(lane < 96, kv, mine).astype(bf16)
        part = pl.ds(4 * h, 4)
        stores.append(pltpu.make_async_copy(send_ref.at[part], send_hbm.at[part], sems.at[13 + h]))
        stores[h].start()
    for store in stores:
        store.wait()


def pick(offsets, x, wq, wk, wv):
    return pl.pallas_call(
        pick_kernel,
        in_specs=[SMEM, HBM, HBM, HBM, HBM],
        out_shape=[
            pltpu.HBM((SHARDS, PICKED, 128), bf16),
            pltpu.VMEM((SEG, D), bf16),
        ],
        out_specs=[HBM, VMEM],
        scratch_shapes=[
            pltpu.VMEM((3, D, D), bf16),
            pltpu.VMEM((SEG, D), bf16),
            pltpu.VMEM((SHARDS, PICKED, 128), bf16),
            pltpu.SemaphoreType.DMA((29,)),
        ],
        compiler_params=pltpu.CompilerParams(vmem_limit_bytes=24 << 20),
        name="pick",
    )(hbm(offsets), hbm(x), hbm(wq), hbm(wk), hbm(wv))


def local_kernel(first, groups, rank_ref, count_ref, off_ref, x_ref, wq_hbm, wk_hbm, wv_hbm, *refs):
    step = pl.program_id(0)
    if first == 0:
        cot_hbm, attn_ref, so_ref, sl_ref, out_hbm, w_ref, o_s, l_s, cot_s, out_s, sems = refs
        load = pltpu.make_async_copy(cot_hbm, cot_s, sems.at[18])
        store = pltpu.make_async_copy(out_s, out_hbm, sems.at[19])
    else:
        attn_ref, so_ref, sl_ref, w_ref, o_s, l_s, sems = refs
    tiles = {g: [3 * g // 2, 3 * g // 2 + 1] for g in range(first, first + groups)}
    windows = {}
    for g, new in tiles.items():
        for u in new:
            if u not in windows:
                r = pl.ds(128 * u, 128)
                windows[u] = (g - first, [
                    pltpu.make_async_copy(hbm.at[:, r], w_ref.at[n, :, r], sems.at[3 * u + n])
                    for n, hbm in enumerate((wq_hbm, wk_hbm, wv_hbm))
                ])

    @pl.when(step == 0)
    def _():
        for _, copies in windows.values():
            for copy in copies:
                copy.start()
        if first == 0:
            load.start()

    for at, copies in windows.values():

        @pl.when(step == at)
        def _(copies=copies):
            for copy in copies:
                copy.wait()

    here = 2 * step
    g = step + first
    t = (3 * g) // 2
    shift = 192 * g - 128 * t
    wl = lanes((D, 128))
    weights = []
    for part in range(2):
        for n in range(3):
            w = w_ref[n, :, pl.ds(pl.multiple_of(128 * t, 128), 256)].astype(f32)
            w = pltpu.roll(w, 256 - 96 * part - shift, 1)[:, :128]
            weights.append(jnp.where(wl < 96, w, 0.0).astype(bf16))
    qkv = nn(x_ref[...], jnp.concatenate(weights, axis=1))
    lane = lanes((SEG, 128))
    live = rows((SEG, 128)) + rank_ref[0] * SEG < count_ref[0]
    bias = jnp.where(live, 0.0, FLOOR)
    ones = jnp.ones((SEG, 128), f32)
    bl = lanes((256, 128))
    sel = lanes((PICKED, 128)) < 48
    for part in range(2):
        qf, kf, vf = (qkv[:, 384 * part + 128 * n : 384 * part + 128 * n + 128] for n in range(3))
        q = jnp.where(lane == 96, 1.0, qf).astype(bf16)
        kf = jnp.where(lane == 96, bias, kf)
        v = jnp.concatenate([vf, ones], axis=1).astype(bf16)
        inside = (lane < 48, (lane >= 48) & (lane < 96))
        kh = [jnp.where(i | (lane == 96), kf, 0.0).astype(bf16) for i in inside]
        for b in range(4):
            r = slice(256 * b, 256 * b + 256)
            both = []
            for a in range(2):
                s = nt(q[r], kh[a])
                m = jnp.max(s, axis=1, keepdims=True)
                e = jnp.exp2((s - m) * SCALE2).astype(bf16)
                o = nn(e, v)
                total = o[:, 128:256]
                both.append((o[:, 0:128] / total, m * SCALE2 + jnp.log2(total)))
            out = jnp.where(bl < 48, both[0][0], both[1][0])
            attn_ref[part, r, :] = out.astype(bf16)
            o_s[part, r, :] = out
            l_s[part, r, :] = jnp.where(bl < 48, both[0][1], both[1][1])
        even = pl.ds(off_ref[4 * g + 2 * part], PICKED, stride=RATE)
        odd = pl.ds(off_ref[4 * g + 2 * part + 1], PICKED, stride=RATE)
        so_ref[here + part] = jnp.where(sel, o_s[part, even, :], o_s[part, odd, :])
        sl_ref[here + part] = jnp.where(sel, l_s[part, even, :], l_s[part, odd, :])


    if first == 0:

        @pl.when(step == 1)
        def _():
            load.wait()
            reorder_cotangent(rank_ref[0], cot_s, out_s)
            store.start()

        @pl.when(step == groups - 1)
        def _():
            store.wait()


def reorder_cotangent(rank, cot_ref, out_ref):
    y, c = rank // 16, rank % 2
    n = rows((96, D))
    offset = lanes((96, D)) - n - 12 * ((n * 171) // 2048)

    def half(i, carry):
        blocks = []
        for k in range(4):
            owner = ((y + k) % 4) * 16 + (c + i) % 2
            blocks.append((offset == 12 * owner).astype(f32))
        onehot = jnp.concatenate(blocks, axis=0).astype(bf16)
        out_ref[pl.ds(pl.multiple_of(384 * i, 384), 384), :] = nt(onehot, cot_ref[...]).astype(bf16)
        return carry

    lax.fori_loop(0, 2, half, 0)


def local(first, groups, rank, count, offsets, x, weights, cot=None):
    out_specs = [pl.BlockSpec((2, SEG, 128), lambda p: (p, 0, 0)), VMEM, VMEM]
    out_shape = [
        pltpu.HBM((2 * groups, SEG, 128), bf16),
        pltpu.VMEM((2 * groups, PICKED, 128), f32),
        pltpu.VMEM((2 * groups, PICKED, 128), f32),
    ]
    scratch = [pltpu.VMEM((3, D, D), bf16), pltpu.VMEM((2, SEG, 128), f32), pltpu.VMEM((2, SEG, 128), f32)]
    if first:
        out_specs[0] = VMEM
        out_shape[0] = pltpu.VMEM((2 * groups, SEG, 128), bf16)
    operands = (rank, count, offsets, vmem(x), *(hbm(w) for w in weights))
    in_specs = [SMEM, SMEM, SMEM, VMEM, HBM, HBM, HBM]
    if first == 0:
        out_specs.append(HBM)
        out_shape.append(pltpu.HBM((D, SEG), bf16))
        scratch += [pltpu.VMEM((SEG, D), bf16), pltpu.VMEM((D, SEG), bf16)]
        operands += (hbm(cot),)
        in_specs.append(HBM)
    scratch.append(pltpu.SemaphoreType.DMA((20,)))
    return pl.pallas_call(
        functools.partial(local_kernel, first, groups),
        grid=(groups,),
        in_specs=in_specs,
        out_specs=out_specs,
        out_shape=out_shape,
        scratch_shapes=scratch,
        compiler_params=pltpu.CompilerParams(
            dimension_semantics=("arbitrary",), vmem_limit_bytes=LOCAL_VMEM
        ),
        cost_estimate=pl.CostEstimate(flops=6_000_000_000 * groups, transcendentals=groups << 22, bytes_accessed=8 << 20),
        name="local",
    )(*operands)


def far_kernel(rank_ref, count_ref, off_ref, recv_ref, ret_ref, after_ref, kb_s, v_s, q_s):
    after_ref[0] = count_ref[0]
    kv = recv_ref[...].reshape(SHARDS * PICKED, 128).astype(f32)
    lane = lanes(kv.shape)
    live = rows(kv.shape) * RATE + off_ref[rank_ref[0] // 4] < count_ref[0]
    kb_s[...] = jnp.where(lane == 112, jnp.where(live, 0.0, FLOOR), kv).astype(bf16)
    v_s[:, 0:128] = kv.astype(bf16)
    v_s[:, 128:256] = jnp.ones(kv.shape, bf16)
    low = recv_ref[:, 0:16, :].reshape(SEG, 128).astype(f32)
    high = recv_ref[:, 16:32, :].reshape(SEG, 128).astype(f32)
    ql = lanes((SEG, 128))
    q = jnp.where(ql < 32, pltpu.roll(low, 32, 1), pltpu.roll(high, 64, 1))
    q_s[...] = jnp.where(ql < 48, q, jnp.where(ql == 112, 1.0, 0.0)).astype(bf16)
    bl = lanes((256, 128))
    hl = lanes((16, 8, 128))
    for b in range(4):
        s = nt(q_s[256 * b : 256 * b + 256, :], kb_s[...])
        m = jnp.max(s, axis=1, keepdims=True)
        e = jnp.exp2((s - m) * SCALE2).astype(bf16)
        o = nn(e, v_s[...])
        total = o[:, 128:256]
        out = pltpu.roll(o[:, 0:128] / total, 80, 1)
        level = m * SCALE2 + jnp.log2(total)
        part0 = level.astype(bf16).astype(f32)
        part1 = (level - part0).astype(bf16).astype(f32)
        part2 = level - part0 - part1
        out = jnp.where(bl < 48, out, jnp.where(bl == 48, part0, jnp.where(bl == 49, part1, part2)))
        out = out.reshape(16, 16, 128)
        second = pltpu.roll(out[:, 8:16, :], 64, 2)
        ret_ref[16 * b : 16 * b + 16] = jnp.where(hl < 64, out[:, 0:8, :], second).astype(bf16)


def far(rank, count, offsets, recv):
    return pl.pallas_call(
        far_kernel,
        in_specs=[SMEM, SMEM, SMEM, VMEM],
        out_specs=[VMEM, SMEM],
        out_shape=[jax.ShapeDtypeStruct((SHARDS, 8, 128), bf16), jax.ShapeDtypeStruct((1,), jnp.int32)],
        scratch_shapes=[
            pltpu.VMEM((SHARDS * PICKED, 128), bf16),
            pltpu.VMEM((SHARDS * PICKED, 256), bf16),
            pltpu.VMEM((SEG, 128), bf16),
        ],
        compiler_params=pltpu.CompilerParams(vmem_limit_bytes=32 << 20),
        cost_estimate=pl.CostEstimate(flops=6_000_000_000, transcendentals=4 << 20, bytes_accessed=2 << 20),
        name="far",
    )(rank, count, offsets, recv)


def natural(pair, n):
    lane = lanes((n, 128))
    out = []
    for t in range(6):
        p = 128 * t // 96
        o = 128 * t - 96 * p
        n0 = 96 - o
        a = pair(p)
        a = pltpu.roll(a, 128 - o, 1) if o else a
        out.append(jnp.where(lane < n0, a, pltpu.roll(pair(p + 1), n0, 1)))
    return jnp.concatenate(out, axis=1)


def merge_kernel(split, rank_ref, count_ref, off_ref, attn0_hbm, attn1_ref, so0_ref, so1_ref, sl0_ref, sl1_ref, ret_ref, cot_hbm, attn_hbm, grad_ref, near_s, cot_s, attn_s, sems):
    loads = []
    for b in range(4):
        part = pl.ds(256 * b, 256)
        loads.append(pltpu.make_async_copy(attn0_hbm.at[:, part], near_s.at[:, part], sems.at[6 + b]))
    last_load = pltpu.make_async_copy(cot_hbm, cot_s, sems.at[5])
    for copy in (*loads, last_load):
        copy.start()
    either = lambda early, late, p: early.at[p] if p < split else late.at[p - split]
    lane = lanes((PICKED, 128))
    merged = []
    for p in range(PAIRS):
        tiles, levels = [], []
        for h in (2 * p, 2 * p + 1):
            pieces = []
            for j in range(4):
                block = ret_ref[4 * h + j].astype(f32)
                pieces += [block, pltpu.roll(block, 64, 1)]
            tile = jnp.concatenate(pieces, axis=0)
            tiles.append(tile)
            levels.append(tile[:, 48:49] + tile[:, 49:50] + tile[:, 50:51])
        value = jnp.where(lane < 48, tiles[0], pltpu.roll(tiles[1], 48, 1))
        gap = jnp.where(lane < 48, levels[0], levels[1]) - either(sl0_ref, sl1_ref, p)[...]
        near = 1.0 / (1.0 + jnp.exp2(gap))
        distant = 1.0 / (1.0 + jnp.exp2(-gap))
        merged.append(near * either(so0_ref, so1_ref, p)[...] + distant * value)
    sel = natural(lambda p: merged[p], PICKED).astype(bf16)
    col = lanes((8, D))
    offcol = jnp.zeros((8, D), jnp.int32)
    for h in range(HEADS):
        offcol = jnp.where(col >= HEAD * h, off_ref[h], offcol)
    offcol = offcol[0:1]
    stores = []
    for b in range(4):
        r = slice(256 * b, 256 * b + 256)
        spread = (rows((256, PICKED)) // RATE + 16 * b == lanes((256, PICKED))).astype(bf16)
        far_rows = nn(spread, sel)
        loads[b].wait()
        near_rows = natural(lambda p: either(near_s, attn1_ref, p)[r, :].astype(f32), 256)
        row = rows((256, D))
        attn = jnp.where(row % RATE == offcol, far_rows, near_rows)
        attn = jnp.where(row + (rank_ref[0] * SEG + 256 * b) < count_ref[0], attn, 0.0).astype(bf16)
        attn_s[r, :] = attn
        part = pl.ds(256 * b, 256)
        stores.append(pltpu.make_async_copy(attn_s.at[part], attn_hbm.at[part], sems.at[b]))
        stores[b].start()
    last_load.wait()

    def half(i, carry):
        part = pl.ds(pl.multiple_of(384 * i, 384), 384)
        grad_ref[part, :] = nn(cot_s[part, :], attn_s[...]).astype(bf16)
        return carry

    lax.fori_loop(0, 2, half, 0)
    for store in stores:
        store.wait()


def merge(rank, count, offsets, near0, near1, ret, cot):
    split = near0[0].shape[0]
    return pl.pallas_call(
        functools.partial(merge_kernel, split),
        in_specs=[SMEM] * 3 + [HBM] + [VMEM] * 6 + [HBM],
        out_specs=[HBM, VMEM],
        out_shape=[pltpu.HBM((SEG, D), bf16), jax.ShapeDtypeStruct((D, D), bf16)],
        scratch_shapes=[
            pltpu.VMEM((split, SEG, 128), bf16),
            pltpu.VMEM((D, SEG), bf16),
            pltpu.VMEM((SEG, D), bf16),
            pltpu.SemaphoreType.DMA((14,)),
        ],
        compiler_params=pltpu.CompilerParams(vmem_limit_bytes=20 << 20),
        cost_estimate=pl.CostEstimate(flops=4_000_000_000, transcendentals=0, bytes_accessed=8 << 20),
        name="merge",
    )(rank, count, offsets, hbm(near0[0]), vmem(near1[0]), *(vmem(a) for n in (1, 2) for a in (near0[n], near1[n])), vmem(ret), hbm(cot))


def branch_kernel(attn_ref, wout_ref, branch_ref):
    branch_ref[...] = nn(attn_ref[...], wout_ref[...]).astype(bf16)


def project_out(attn, wout):
    rows_of = pl.BlockSpec((256, D), lambda b: (b, 0))
    return pl.pallas_call(
        branch_kernel,
        grid=(4,),
        in_specs=[rows_of, pl.BlockSpec((D, D), lambda b: (0, 0))],
        out_specs=rows_of,
        out_shape=jax.ShapeDtypeStruct((SEG, D), bf16),
        compiler_params=pltpu.CompilerParams(dimension_semantics=("arbitrary",), vmem_limit_bytes=BRANCH_VMEM),
        cost_estimate=pl.CostEstimate(flops=1_300_000_000, transcendentals=0, bytes_accessed=5 << 20),
        name="branch",
    )(hbm(attn), hbm(wout))


def place(y, z, c):
    return (y * 8 + z) * 2 + c


EVERY = [(y, z, c) for y in range(4) for z in range(8) for c in range(2)]
Z_GROUPS = [[place(y, z, c) for z in range(8)] for y in range(4) for c in range(2)]


def to_partner(a):
    return lax.ppermute(a, "seq", [(place(y, z, c), place(y, z, 1 - c)) for y, z, c in EVERY])


def along_y(a, k):
    return lax.ppermute(a, "seq", [(place(y, z, c), place((y + k) % 4, z, c)) for y, z, c in EVERY])


def across_slides(a, k):
    return lax.ppermute(a, "dp", [(x, x ^ k) for x in range(4)])


def reduce_gradient(grad):
    got = to_partner(grad[D // 2 :])
    half = (grad[: D // 2].astype(f32) + got.astype(f32)).astype(bf16)
    blocks = [half[96 * k : 96 * k + 96] for k in (1, 2, 3)]
    got = [along_y(blocks[k - 1], k) for k in (1, 2, 3)]
    part = half[:96].astype(f32) + got[0].astype(f32) + (got[1].astype(f32) + got[2].astype(f32))
    blocks = part.astype(bf16).reshape(8, 12, D)
    blocks = lax.all_to_all(blocks, "seq", 0, 0, tiled=True, axis_index_groups=Z_GROUPS)
    mine = blocks.astype(f32).sum(axis=0)
    got = [across_slides(mine, k) for k in (1, 2, 3)]
    return ((mine + got[0]) + (got[1] + got[2])).T


def body(tiles, tile_count, offsets, w_query, w_key, w_value, w_out, cotangent):
    x = tiles[0]
    rank = lax.axis_index("seq")
    rank = rank.astype(jnp.int32)[None]
    weights = (w_query, w_key, w_value)
    send, x = pick(offsets, x, *weights)
    recv = lax.all_to_all(send, "seq", 0, 0, tiled=True)
    *near0, cot = local(0, EARLY, rank, tile_count, offsets, x, weights, cotangent[0])
    ret, after = far(rank, tile_count, offsets, recv)
    back = lax.all_to_all(ret, "seq", 0, 0, tiled=True)
    near1 = local(EARLY, 4 - EARLY, rank, after, offsets, x, weights)
    attn, grad = merge(rank, tile_count, offsets, near0, near1, back, cot)
    branch = project_out(attn, w_out)
    return branch[None], reduce_gradient(grad)


def solution(mesh):
    in_specs = (P("dp", "seq", None), P("dp"), P(), P(), P(), P(), P(), P("dp", "seq", None))
    out_specs = (P("dp", "seq", None), P(None, "seq"))
    return jax.shard_map(body, mesh=mesh, in_specs=in_specs, out_specs=out_specs, check_vma=False)
```
